32 devices in a mesh: kpt: 2 (over y), row: 8 (over z, x), freq: 2 (over core).
Axes of the slice: x: 2, y: 2, z: 4, core: 2. Of those that a mesh axis runs over, the one named last changes fastest.
Arguments:
- screened: bfloat16 [8, 2, 8192, 8192], P(('kpt', 'freq'), None, 'row'), parts along dimension 0, may hold values from -0.0625 to 0.0625
- elements: bfloat16 [2, 1024, 8192], P(None, 'kpt', 'row'), parts along dimension 1, may hold values from -0.59765625 to 0.59765625
- node_freq: float32 [4], P('freq'), may hold values from 0.1 to 2
- node_weight: float32 [4], P('freq'), may hold values from 0.1 to 1
- band_energy: float32 [1024], P('kpt'), parts along dimension 0, may hold values from -1 to 1
- energy_grid: float32 [64], replicated, may hold values from -1 to 1
- pair_state: int32 [1024], P('kpt'), parts along dimension 0, may hold values from 0 to 31
- pair_band: int32 [1024], P('kpt'), parts along dimension 0, may hold values from 0 to 511
Outputs:
- sigma: float32 [2, 64, 64], P(None, 'kpt'), parts along dimension 1
The draws below stay inside these ranges and needn't reach their ends.
There are 2 independent parts, one for each index of `kpt`. The reference program is written for one: setup_inputs(seed, part) draws one part's arguments, and reference() takes and returns one part's arrays. A program takes and returns all parts, laid end to end along the dimension named above; an argument that names none is the same for every part. Nothing has to cross between parts.
All inputs are finite; a program needn't handle non-finite values.
Results may differ from the reference program's by a relative error of at most 0.0003.
Values may be sent and summed in bfloat16 or wider, within the bound.
A program may use at most 192 MiB of HBM per device.

```python
import math
import jax
import jax.numpy as jnp

NG = 8192
NPAIR = 512
NBAND = 512
NSTATE = 32
NE = 64
NODES = 4


def place_ends(result, key, low, largest):
    spot = [jax.random.randint(jax.random.fold_in(key, axis), (), 0, length) for axis, length in enumerate(result.shape)]
    main_axis = result.shape.index(max(result.shape))
    neighbour = spot[:main_axis] + [(spot[main_axis] + 1) % result.shape[main_axis]] + spot[main_axis + 1:]
    return result.at[tuple(spot)].set(low).at[tuple(neighbour)].set(largest)


def steps_of(own_key, shape, split, low, high):
    def one(dim, shards_of):
        steps = jax.random.uniform(jax.random.fold_in(jax.random.fold_in(own_key, 6), dim), (shards_of,), jnp.float32, low / len(split), high / len(split))
        return jnp.repeat(jnp.exp(steps), shape[dim] // shards_of).reshape((-1,) + (1,) * (len(shape) - dim - 1))

    loudness = one(*split[0])
    for cut in split[1:]:
        loudness = loudness * one(*cut)
    return loudness


def centred(key, extent, scale, most, shards=(), kind=jnp.bfloat16):
    result = scale * jax.random.normal(key, extent, jnp.float32)
    if shards:
        result = result * steps_of(key, extent, shards, -0.22, 0.18)
    return jnp.clip(result, -most, most).astype(kind)


def setup_inputs(seed: int = 0, part: int = 0) -> dict:
    key_of = jax.random.split(jax.random.key(seed), 9)
    part_splits = jax.random.split(jax.random.fold_in(key_of[8], part), 9)
    return {
        "screened": centred(part_splits[0], (NODES, 2, NG, NG), NG ** -0.5, 0.0625, ((0, 2), (2, 8))),
        "elements": centred(part_splits[1], (2, NPAIR, NG), 0.1, 0.59765625, ((2, 8),)),
        "node_freq": jnp.clip(jnp.exp(math.log(2.0) - 2.9957323 * jax.random.uniform(key_of[2], (NODES,), jnp.float32) ** steps_of(key_of[2], (NODES,), ((0, 2),), -0.2, 0.2)), 0.1, 2.0),
        "node_weight": jnp.clip(jnp.exp(math.log(1.0) - 2.3025851 * jax.random.uniform(key_of[3], (NODES,), jnp.float32) ** steps_of(key_of[3], (NODES,), ((0, 2),), -0.2, 0.2)), 0.1, 1.0),
        "band_energy": jnp.clip(jax.random.uniform(part_splits[4], (NBAND,), jnp.float32, -1.0, 1.0), -1.0, 1.0),
        "energy_grid": jnp.clip(jax.random.uniform(key_of[5], (NE,), jnp.float32, -1.0, 1.0), -1.0, 1.0),
        "pair_state": place_ends(jax.random.randint(part_splits[6], (NPAIR,), 0, NSTATE), jax.random.fold_in(part_splits[6], 1), 0, NSTATE - 1).astype(jnp.int32),
        "pair_band": place_ends(jax.random.randint(part_splits[7], (NPAIR,), 0, NBAND), jax.random.fold_in(part_splits[7], 1), 0, NBAND - 1).astype(jnp.int32),
    }


def reference(screened, elements, node_freq, node_weight, band_energy, energy_grid, pair_state, pair_band):
    real_el = elements[0]
    imag_el = elements[1]
    real_t = real_el.T.astype(jnp.float32)
    imag_t = imag_el.T.astype(jnp.float32)
    forms_re = []
    forms_im = []
    for node in range(NODES):
        w_real = screened[node, 0]
        w_imag = screened[node, 1]
        y_real = jnp.dot(w_real, real_el.T, preferred_element_type=jnp.float32) - jnp.dot(w_imag, imag_el.T, preferred_element_type=jnp.float32)
        y_imag = jnp.dot(w_real, imag_el.T, preferred_element_type=jnp.float32) + jnp.dot(w_imag, real_el.T, preferred_element_type=jnp.float32)
        forms_re.append(jnp.sum(real_t * y_real + imag_t * y_imag, axis=0))
        forms_im.append(jnp.sum(real_t * y_imag - imag_t * y_real, axis=0))
    form_re = jnp.stack(forms_re)
    form_im = jnp.stack(forms_im)
    pair_eps = band_energy[pair_band]
    delta = energy_grid[None, :] - pair_eps[:, None]
    factor = node_weight[:, None, None] * delta[None] / (delta[None] ** 2 + node_freq[:, None, None] ** 2)
    terms_re = jnp.sum(form_re[:, :, None] * factor, axis=0)
    terms_im = jnp.sum(form_im[:, :, None] * factor, axis=0)
    sig_re = jax.ops.segment_sum(terms_re, pair_state, NSTATE)
    sig_im = jax.ops.segment_sum(terms_im, pair_state, NSTATE)
    return jnp.stack([sig_re, sig_im])
```

```python
import functools

import jax
import jax.numpy as jnp
from jax import lax
from jax.experimental import pallas as pl
from jax.experimental.pallas import tpu as pltpu
from jax.sharding import PartitionSpec as P

NSTATE = 32
TILE = 512


def product(weights, piece):
    return jnp.einsum("jgc,pc->jgp", weights, piece, preferred_element_type=jnp.float32)


def self_energy(
    form_re, form_im, node_freq, node_weight, band_energy, energy_grid, pair_state, pair_band
):
    band_onehot = (
        pair_band[:, None] == jnp.arange(band_energy.shape[0], dtype=jnp.int32)[None, :]
    ).astype(jnp.float32)
    pair_eps = jnp.dot(band_onehot, band_energy, precision=lax.Precision.HIGHEST)
    delta = energy_grid[None, :] - pair_eps[:, None]
    factor = (
        node_weight[:, None, None]
        * delta[None]
        / (delta[None] ** 2 + node_freq[:, None, None] ** 2)
    )
    terms_re = jnp.sum(form_re[:, :, None] * factor, axis=0)
    terms_im = jnp.sum(form_im[:, :, None] * factor, axis=0)
    state_onehot = (jnp.arange(NSTATE, dtype=jnp.int32)[:, None] == pair_state[None, :]).astype(
        jnp.float32
    )
    sig_re = jnp.dot(state_onehot, terms_re, precision=lax.Precision.HIGHEST)
    sig_im = jnp.dot(state_onehot, terms_im, precision=lax.Precision.HIGHEST)
    return jnp.stack([sig_re, sig_im])


def ring_position(idx, n):
    par = idx % 2
    return (1 - par) * (idx // 2) + par * (n - 1 - idx // 2)


def ring_index(pos, n):
    high = pos // (n // 2)
    return (1 - high) * (2 * pos) + high * (2 * (n - 1 - pos) + 1)


def ring_kernel(
    n, nodes, rows, chunk, wide, tile, depth,
    w_hbm, m_hbm, out_ref,
    held, wbuf, rhs, own_sem, w_sem, send_sem, recv_sem, sib_send, sib_recv,
):
    me = lax.axis_index("row")
    core = lax.axis_index("freq")
    pos = ring_position(me, n)
    right = ring_index((pos + 1) % n, n)
    left = ring_index((pos + n - 1) % n, n)
    other = 1 - core
    half = wide // 2
    units = 2 * n

    def item(step, way):
        hop = (step + 1) // 2
        first = (step + 1) % 2
        owner_pos = (pos + n + (2 * way - 1) * hop) % n
        part = (1 - way) * first + way * (1 - first)
        return ring_index(owner_pos, n), part

    def w_copies(unit):
        owner, part = item(unit // 2, unit % 2)
        slot = unit % depth
        start = pl.multiple_of(owner * 2 * chunk + part * chunk, 128)
        return [
            pltpu.make_async_copy(
                w_hbm.at[j, c, :, pl.ds(start, chunk)],
                wbuf.at[slot, j, :, pl.ds(c * chunk, chunk)],
                w_sem.at[slot, j, c],
            )
            for j in range(nodes)
            for c in range(2)
        ]

    def send(step, way, owner, part):
        ref = held.at[owner, part, core]
        return pltpu.make_async_remote_copy(
            src_ref=ref,
            dst_ref=ref,
            send_sem=send_sem.at[step, way],
            recv_sem=recv_sem.at[step, way],
            device_id={"row": right if way == 0 else left},
            device_id_type=pl.DeviceIdType.MESH,
        )

    def pass_over(step, way, owner, part, core_of):
        ref = held.at[owner, part, core_of]
        return pltpu.make_async_remote_copy(
            src_ref=ref,
            dst_ref=ref,
            send_sem=sib_send.at[step, way],
            recv_sem=sib_recv.at[step, way],
            device_id={"freq": other},
            device_id_type=pl.DeviceIdType.MESH,
        )

    own = pltpu.make_async_copy(m_hbm, held.at[me], own_sem)
    own.start()
    for unit in range(depth - 1):
        for copy in w_copies(unit):
            copy.start()
    barrier = pltpu.get_barrier_semaphore()
    pl.semaphore_signal(barrier, device_id={"row": right}, device_id_type=pl.DeviceIdType.MESH)
    pl.semaphore_signal(barrier, device_id={"row": left}, device_id_type=pl.DeviceIdType.MESH)
    pl.semaphore_signal(barrier, device_id={"freq": other}, device_id_type=pl.DeviceIdType.MESH)
    own.wait()
    pl.semaphore_wait(barrier, 3)
    for step in (1, 2):
        for way in (0, 1):
            part = (step + 1) % 2 if way == 0 else 1 - (step + 1) % 2
            send(step, way, me, part).start()
    out_ref[...] = jnp.zeros_like(out_ref)

    def compute(unit):
        slot = unit % depth
        owner, part = item(unit // 2, unit % 2)
        for f in range(2):
            rhs[f, :chunk, :] = held[owner, part, f]
            rhs[f, chunk:, :half] = -held[owner, part, f, :, half:]
            rhs[f, chunk:, half:] = held[owner, part, f, :, :half]
        for copy in w_copies(unit):
            copy.wait()

        @pl.when(unit + depth - 1 < units)
        def _():
            for copy in w_copies(unit + depth - 1):
                copy.start()

        tiles = rows // tile

        def one(i, carry):
            j = i // (2 * tiles)
            f = (i // tiles) % 2
            t = i % tiles
            spot = pl.ds(pl.multiple_of(t * tile, tile), tile)
            y = jnp.dot(wbuf[slot, j, spot, :], rhs[f], preferred_element_type=jnp.float32)
            per = chunk // tile
            mine = pl.ds(pl.multiple_of((t % per) * tile, tile), tile)
            m = held[me, t // per, f, mine, :].astype(jnp.float32)
            r, s = m[:, :half], m[:, half:]
            yr, yi = y[:, :half], y[:, half:]
            out_ref[0, j, f] += jnp.sum((r * yr + s * yi).reshape(tile // 8, 8, half), axis=0)
            out_ref[1, j, f] += jnp.sum((r * yi - s * yr).reshape(tile // 8, 8, half), axis=0)
            return carry

        lax.fori_loop(0, nodes * 2 * tiles, one, 0)

    def step_body(step, carry):
        @pl.when(step >= 1)
        def _():
            for way in (0, 1):
                owner, part = item(step, way)
                send(step, way, owner, part).wait_recv()

                @pl.when(step + 2 < n)
                def _():
                    send(step + 2, way, owner, part).start()

                pass_over(step, way, owner, part, core).start()
            for way in (0, 1):
                owner, part = item(step, way)
                pass_over(step, way, owner, part, other).wait_recv()

        def each(way, c):
            compute(2 * step + way)
            return c

        lax.fori_loop(0, 2, each, 0)
        return carry

    lax.fori_loop(0, n, step_body, 0)

    def drain(step, carry):
        for way in (0, 1):
            owner, part = item(step, way)
            send(step, way, owner, part).wait_send()
            pass_over(step, way, owner, part, core).wait_send()
        return carry

    lax.fori_loop(1, n, drain, 0)


def ring_forms(screened, elements):
    nodes, _, rows, ng = screened.shape
    n = lax.axis_size("row")
    npair = elements.shape[1]
    block = elements.shape[2]
    chunk = block // 2
    wide = npair
    tile = min(TILE, chunk)
    depth = 4
    m = elements.reshape(2, 2, npair // 2, 2, chunk).transpose(3, 1, 4, 0, 2)
    m = m.reshape(2, 2, chunk, wide)
    out = pl.pallas_call(
        functools.partial(ring_kernel, n, nodes, rows, chunk, wide, tile, depth),
        out_shape=jax.ShapeDtypeStruct((2, nodes, 2, 8, npair // 2), jnp.float32),
        in_specs=[pl.BlockSpec(memory_space=pl.ANY)] * 2,
        out_specs=pl.BlockSpec(memory_space=pltpu.VMEM),
        scratch_shapes=[
            pltpu.VMEM((n, 2, 2, chunk, wide), jnp.bfloat16),
            pltpu.VMEM((depth, nodes, rows, 2 * chunk), jnp.bfloat16),
            pltpu.VMEM((2, 2 * chunk, wide), jnp.bfloat16),
            pltpu.SemaphoreType.DMA,
            pltpu.SemaphoreType.DMA((depth, nodes, 2)),
            pltpu.SemaphoreType.DMA((n, 2)),
            pltpu.SemaphoreType.DMA((n, 2)),
            pltpu.SemaphoreType.DMA((n, 2)),
            pltpu.SemaphoreType.DMA((n, 2)),
        ],
        compiler_params=pltpu.CompilerParams(
            collective_id=0, has_side_effects=True, vmem_limit_bytes=60 * 1024 * 1024
        ),
    )(screened, m)
    forms = jnp.sum(out, axis=3).reshape(2, nodes, npair)
    return forms[0], forms[1]


def per_device(
    screened, elements, node_freq, node_weight, band_energy, energy_grid, pair_state, pair_band
):
    n = lax.axis_size("row")
    if n >= 4 and n % 2 == 0 and elements.shape[2] % 256 == 0 and elements.shape[1] % 256 == 0:
        form_re, form_im = ring_forms(screened, elements)
        partial_sigma = self_energy(
            form_re, form_im, node_freq, node_weight, band_energy, energy_grid, pair_state,
            pair_band,
        )
        return lax.psum(partial_sigma, ("row", "freq"))
    w_real = screened[:, 0]
    w_imag = screened[:, 1]
    npair = elements.shape[1]
    half = npair // lax.axis_size("freq")
    mine = lax.dynamic_slice_in_dim(elements, lax.axis_index("freq") * half, half, 1)
    collected = lax.all_gather(mine, "row", axis=2, tiled=True)
    piece = lax.all_gather(collected, "freq", axis=1, tiled=True)
    part_real = product(w_real, piece[0]) - product(w_imag, piece[1])
    part_imag = product(w_real, piece[1]) + product(w_imag, piece[0])
    stacked = jnp.stack([part_real, part_imag])
    y_real = stacked[0]
    y_imag = stacked[1]
    own_real = elements[0].T.astype(jnp.float32)[None]
    own_imag = elements[1].T.astype(jnp.float32)[None]
    form_re = jnp.sum(own_real * y_real + own_imag * y_imag, axis=1)
    form_im = jnp.sum(own_real * y_imag - own_imag * y_real, axis=1)
    form_re, form_im = lax.psum((form_re, form_im), "row")
    partial_sigma = self_energy(
        form_re, form_im, node_freq, node_weight, band_energy, energy_grid, pair_state, pair_band
    )
    return lax.psum(partial_sigma, "freq")


def solution(mesh):
    in_specs = (
        P(("kpt", "freq"), None, "row", None),
        P(None, "kpt", "row"),
        P("freq"),
        P("freq"),
        P("kpt"),
        P(),
        P("kpt"),
        P("kpt"),
    )
    out_specs = P(None, "kpt", None)
    return jax.shard_map(
        per_device, mesh=mesh, in_specs=in_specs, out_specs=out_specs, check_vma=False
    )
```

```python
import functools

import jax
import jax.numpy as jnp
from jax import lax
from jax.experimental import pallas as pl
from jax.experimental.pallas import tpu as pltpu
from jax.sharding import PartitionSpec as P

NSTATE = 32
TILE = 512
DEPTH = 4


def product(weights, piece):
    return jnp.einsum("jgc,pc->jgp", weights, piece, preferred_element_type=jnp.float32)


def self_energy(
    form_re, form_im, node_freq, node_weight, band_energy, energy_grid, pair_state, pair_band
):
    band_onehot = (
        pair_band[:, None] == jnp.arange(band_energy.shape[0], dtype=jnp.int32)[None, :]
    ).astype(jnp.float32)
    pair_eps = jnp.dot(band_onehot, band_energy, precision=lax.Precision.HIGHEST)
    delta = energy_grid[None, :] - pair_eps[:, None]
    factor = (
        node_weight[:, None, None]
        * delta[None]
        / (delta[None] ** 2 + node_freq[:, None, None] ** 2)
    )
    terms_re = jnp.sum(form_re[:, :, None] * factor, axis=0)
    terms_im = jnp.sum(form_im[:, :, None] * factor, axis=0)
    state_onehot = (jnp.arange(NSTATE, dtype=jnp.int32)[:, None] == pair_state[None, :]).astype(
        jnp.float32
    )
    sig_re = jnp.dot(state_onehot, terms_re, precision=lax.Precision.HIGHEST)
    sig_im = jnp.dot(state_onehot, terms_im, precision=lax.Precision.HIGHEST)
    return jnp.stack([sig_re, sig_im])


def ring_position(idx, n):
    par = idx % 2
    return (1 - par) * (idx // 2) + par * (n - 1 - idx // 2)


def ring_index(pos, n):
    high = pos // (n // 2)
    return (1 - high) * (2 * pos) + high * (2 * (n - 1 - pos) + 1)


def ring_kernel(
    n, nodes, rows, chunk, wide, tile, depth,
    w_hbm, m_hbm, param_ref, out_ref,
    block, held, wbuf, rhs, acc, forms, peers, twin,
    own_sem, w_sem, send_sem, recv_sem, sib_send, sib_recv,
    form_send, form_recv, twin_send, twin_recv,
):
    me = lax.axis_index("row")
    core = lax.axis_index("freq")
    pos = ring_position(me, n)
    right = ring_index((pos + 1) % n, n)
    left = ring_index((pos + n - 1) % n, n)
    other = 1 - core
    half = wide // 2
    units = 2 * n

    def item(step, way):
        hop = (step + 1) // 2
        first = (step + 1) % 2
        owner_pos = (pos + n + (2 * way - 1) * hop) % n
        part = (1 - way) * first + way * (1 - first)
        return ring_index(owner_pos, n), part

    def w_copies(unit):
        owner, part = item(unit // 2, unit % 2)
        slot = unit % depth
        start = pl.multiple_of(owner * 2 * chunk + part * chunk, 128)
        return [
            pltpu.make_async_copy(
                w_hbm.at[j, c, :, pl.ds(start, chunk)],
                wbuf.at[slot, j, :, pl.ds(c * chunk, chunk)],
                w_sem.at[slot, j, c],
            )
            for j in range(nodes)
            for c in range(2)
        ]

    def send(step, way, owner, part):
        ref = held.at[owner, part, core]
        return pltpu.make_async_remote_copy(
            src_ref=ref,
            dst_ref=ref,
            send_sem=send_sem.at[step, way],
            recv_sem=recv_sem.at[step, way],
            device_id={"row": right if way == 0 else left},
            device_id_type=pl.DeviceIdType.MESH,
        )

    def pass_over(step, way, owner, part, core_of):
        ref = held.at[owner, part, core_of]
        return pltpu.make_async_remote_copy(
            src_ref=ref,
            dst_ref=ref,
            send_sem=sib_send.at[step, way],
            recv_sem=sib_recv.at[step, way],
            device_id={"freq": other},
            device_id_type=pl.DeviceIdType.MESH,
        )

    own = pltpu.make_async_copy(m_hbm, block, own_sem)
    own.start()
    for unit in range(depth - 1):
        for copy in w_copies(unit):
            copy.start()
    barrier = pltpu.get_barrier_semaphore()
    for hop in range(1, n):
        pl.semaphore_signal(
            barrier, device_id={"row": (me + hop) % n}, device_id_type=pl.DeviceIdType.MESH
        )
    pl.semaphore_signal(barrier, device_id={"freq": other}, device_id_type=pl.DeviceIdType.MESH)
    own.wait()

    def turn(part, f):
        pairs = pl.ds(pl.multiple_of(f * half, half), half)
        for c in range(2):
            piece = block[c, pairs, part * chunk : (part + 1) * chunk]
            held[me, part, f, :, c * half : (c + 1) * half] = piece.T

    turn(0, core)
    turn(1, core)
    pl.semaphore_wait(barrier, n)
    for step in (1, 2):
        for way in (0, 1):
            part = (step + 1) % 2 if way == 0 else 1 - (step + 1) % 2
            send(step, way, me, part).start()
    turn(0, other)
    turn(1, other)
    acc[...] = jnp.zeros_like(acc)

    def compute(unit):
        slot = unit % depth
        owner, part = item(unit // 2, unit % 2)
        for f in range(2):
            rhs[f, :chunk, :] = held[owner, part, f]
            rhs[f, chunk:, :half] = -held[owner, part, f, :, half:]
            rhs[f, chunk:, half:] = held[owner, part, f, :, :half]
        for copy in w_copies(unit):
            copy.wait()

        @pl.when(unit + depth - 1 < units)
        def _():
            for copy in w_copies(unit + depth - 1):
                copy.start()

        tiles = rows // tile

        def one(i, carry):
            j = i // (2 * tiles)
            f = (i // tiles) % 2
            t = i % tiles
            spot = pl.ds(pl.multiple_of(t * tile, tile), tile)
            y = jnp.dot(wbuf[slot, j, spot, :], rhs[f], preferred_element_type=jnp.float32)
            per = chunk // tile
            mine = pl.ds(pl.multiple_of((t % per) * tile, tile), tile)
            m = held[me, t // per, f, mine, :].astype(jnp.float32)
            r, s = m[:, :half], m[:, half:]
            yr, yi = y[:, :half], y[:, half:]
            acc[0, j, f] += jnp.sum((r * yr + s * yi).reshape(tile // 8, 8, half), axis=0)
            acc[1, j, f] += jnp.sum((r * yi - s * yr).reshape(tile // 8, 8, half), axis=0)
            return carry

        lax.fori_loop(0, nodes * 2 * tiles, one, 0)

    def step_body(step, carry):
        @pl.when(step >= 1)
        def _():
            for way in (0, 1):
                owner, part = item(step, way)
                send(step, way, owner, part).wait_recv()

                @pl.when(step + 2 < n)
                def _():
                    send(step + 2, way, owner, part).start()

                pass_over(step, way, owner, part, core).start()
            for way in (0, 1):
                owner, part = item(step, way)
                pass_over(step, way, owner, part, other).wait_recv()

        def each(way, c):
            compute(2 * step + way)
            return c

        lax.fori_loop(0, 2, each, 0)
        return carry

    lax.fori_loop(0, n, step_body, 0)

    lines = 2 * nodes * 2
    forms[:lines, :] = jnp.sum(acc[...], axis=3).reshape(lines, half)
    forms[lines:, :] = jnp.zeros_like(forms[lines:, :])

    def spread(hop):
        return pltpu.make_async_remote_copy(
            src_ref=forms,
            dst_ref=peers.at[hop - 1],
            send_sem=form_send.at[hop - 1],
            recv_sem=form_recv.at[hop - 1],
            device_id={"row": (me + hop) % n},
            device_id_type=pl.DeviceIdType.MESH,
        )

    for hop in range(1, n):
        spread(hop).start()
    def drain(step, carry):
        for way in (0, 1):
            owner, part = item(step, way)
            send(step, way, owner, part).wait_send()
            pass_over(step, way, owner, part, core).wait_send()
        return carry

    lax.fori_loop(1, n, drain, 0)
    total = forms[...]
    for hop in range(1, n):
        spread(hop).wait()
        total += peers[hop - 1]
    twin[0, :lines, :] = total[:lines, :]
    twin[0, lines:, :] = param_ref[...]
    swap = pltpu.make_async_remote_copy(
        src_ref=twin.at[0],
        dst_ref=twin.at[1],
        send_sem=twin_send,
        recv_sem=twin_recv,
        device_id={"freq": other},
        device_id_type=pl.DeviceIdType.MESH,
    )
    swap.start()
    out_ref[0] = twin[0]
    swap.wait()
    out_ref[1] = twin[1]


def ring_forms(screened, elements, node_freq, node_weight):
    nodes, _, rows, ng = screened.shape
    n = lax.axis_size("row")
    npair = elements.shape[1]
    block = elements.shape[2]
    chunk = block // 2
    half = npair // 2
    tile = min(TILE, chunk)
    depth = DEPTH
    lines = 2 * nodes * 2
    spare = -(-2 * nodes // 8) * 8
    params = jnp.concatenate([node_freq, node_weight])
    params = jnp.pad(params, (0, spare - 2 * nodes))
    params = jnp.broadcast_to(params[:, None], (spare, half))
    out = pl.pallas_call(
        functools.partial(ring_kernel, n, nodes, rows, chunk, npair, tile, depth),
        out_shape=jax.ShapeDtypeStruct((2, lines + spare, half), jnp.float32),
        in_specs=[
            pl.BlockSpec(memory_space=pl.ANY),
            pl.BlockSpec(memory_space=pl.ANY),
            pl.BlockSpec(memory_space=pltpu.VMEM),
        ],
        out_specs=pl.BlockSpec(memory_space=pltpu.VMEM),
        scratch_shapes=[
            pltpu.VMEM((2, npair, block), jnp.bfloat16),
            pltpu.VMEM((n, 2, 2, chunk, npair), jnp.bfloat16),
            pltpu.VMEM((depth, nodes, rows, 2 * chunk), jnp.bfloat16),
            pltpu.VMEM((2, 2 * chunk, npair), jnp.bfloat16),
            pltpu.VMEM((2, nodes, 2, 8, half), jnp.float32),
            pltpu.VMEM((lines + spare, half), jnp.float32),
            pltpu.VMEM((n - 1, lines + spare, half), jnp.float32),
            pltpu.VMEM((2, lines + spare, half), jnp.float32),
            pltpu.SemaphoreType.DMA,
            pltpu.SemaphoreType.DMA((depth, nodes, 2)),
            pltpu.SemaphoreType.DMA((n, 2)),
            pltpu.SemaphoreType.DMA((n, 2)),
            pltpu.SemaphoreType.DMA((n, 2)),
            pltpu.SemaphoreType.DMA((n, 2)),
            pltpu.SemaphoreType.DMA((n - 1,)),
            pltpu.SemaphoreType.DMA((n - 1,)),
            pltpu.SemaphoreType.DMA,
            pltpu.SemaphoreType.DMA,
        ],
        compiler_params=pltpu.CompilerParams(
            collective_id=0, has_side_effects=True, vmem_limit_bytes=62 * 1024 * 1024
        ),
    )(screened, elements, params)
    forms = out[:, :lines].reshape(2, 2, nodes, npair).transpose(1, 0, 2, 3)
    forms = forms.reshape(2, 2 * nodes, npair)
    freqs = out[:, lines : lines + nodes, 0].reshape(-1)
    weights = out[:, lines + nodes : lines + 2 * nodes, 0].reshape(-1)
    return forms[0], forms[1], freqs, weights


def per_device(
    screened, elements, node_freq, node_weight, band_energy, energy_grid, pair_state, pair_band
):
    n = lax.axis_size("row")
    two = n >= 4 and n % 2 == 0 and lax.axis_size("freq") == 2
    if two and elements.shape[2] % 256 == 0 and elements.shape[1] % 256 == 0:
        form_re, form_im, freqs, weights = ring_forms(screened, elements, node_freq, node_weight)
        return self_energy(
            form_re, form_im, freqs, weights, band_energy, energy_grid, pair_state, pair_band
        )
    w_real = screened[:, 0]
    w_imag = screened[:, 1]
    npair = elements.shape[1]
    half = npair // lax.axis_size("freq")
    mine = lax.dynamic_slice_in_dim(elements, lax.axis_index("freq") * half, half, 1)
    collected = lax.all_gather(mine, "row", axis=2, tiled=True)
    piece = lax.all_gather(collected, "freq", axis=1, tiled=True)
    part_real = product(w_real, piece[0]) - product(w_imag, piece[1])
    part_imag = product(w_real, piece[1]) + product(w_imag, piece[0])
    stacked = jnp.stack([part_real, part_imag])
    y_real = stacked[0]
    y_imag = stacked[1]
    own_real = elements[0].T.astype(jnp.float32)[None]
    own_imag = elements[1].T.astype(jnp.float32)[None]
    form_re = jnp.sum(own_real * y_real + own_imag * y_imag, axis=1)
    form_im = jnp.sum(own_real * y_imag - own_imag * y_real, axis=1)
    form_re, form_im = lax.psum((form_re, form_im), "row")
    partial_sigma = self_energy(
        form_re, form_im, node_freq, node_weight, band_energy, energy_grid, pair_state, pair_band
    )
    return lax.psum(partial_sigma, "freq")


def solution(mesh):
    in_specs = (
        P(("kpt", "freq"), None, "row", None),
        P(None, "kpt", "row"),
        P("freq"),
        P("freq"),
        P("kpt"),
        P(),
        P("kpt"),
        P("kpt"),
    )
    out_specs = P(None, "kpt", None)
    return jax.shard_map(
        per_device, mesh=mesh, in_specs=in_specs, out_specs=out_specs, check_vma=False
    )
```

```python
import functools

import jax
import jax.numpy as jnp
from jax import lax
from jax.experimental import pallas as pl
from jax.experimental.pallas import tpu as pltpu
from jax.sharding import PartitionSpec as P

NSTATE = 32
TILE = 512
DEPTH = 4


def product(weights, piece):
    return jnp.einsum("jgc,pc->jgp", weights, piece, preferred_element_type=jnp.float32)


def self_energy(
    form_re, form_im, node_freq, node_weight, band_energy, energy_grid, pair_state, pair_band
):
    band_onehot = (
        pair_band[:, None] == jnp.arange(band_energy.shape[0], dtype=jnp.int32)[None, :]
    ).astype(jnp.float32)
    pair_eps = jnp.dot(band_onehot, band_energy, precision=lax.Precision.HIGHEST)
    delta = energy_grid[None, :] - pair_eps[:, None]
    factor = (
        node_weight[:, None, None]
        * delta[None]
        / (delta[None] ** 2 + node_freq[:, None, None] ** 2)
    )
    terms_re = jnp.sum(form_re[:, :, None] * factor, axis=0)
    terms_im = jnp.sum(form_im[:, :, None] * factor, axis=0)
    state_onehot = (jnp.arange(NSTATE, dtype=jnp.int32)[:, None] == pair_state[None, :]).astype(
        jnp.float32
    )
    sig_re = jnp.dot(state_onehot, terms_re, precision=lax.Precision.HIGHEST)
    sig_im = jnp.dot(state_onehot, terms_im, precision=lax.Precision.HIGHEST)
    return jnp.stack([sig_re, sig_im])


def ring_position(idx, n):
    par = idx % 2
    return (1 - par) * (idx // 2) + par * (n - 1 - idx // 2)


def ring_index(pos, n):
    high = pos // (n // 2)
    return (1 - high) * (2 * pos) + high * (2 * (n - 1 - pos) + 1)


def ring_kernel(
    n, nodes, rows, chunk, wide, tile, depth,
    w_hbm, m_hbm, param_ref, out_ref,
    block, held, wbuf, rhs, acc, forms, peers, twin,
    own_sem, w_sem, send_sem, recv_sem, sib_send, sib_recv,
    form_send, form_recv, twin_send, twin_recv,
):
    me = lax.axis_index("row")
    core = lax.axis_index("freq")
    pos = ring_position(me, n)
    right = ring_index((pos + 1) % n, n)
    left = ring_index((pos + n - 1) % n, n)
    other = 1 - core
    half = wide // 2
    units = 2 * n

    def item(step, way):
        hop = (step + 1) // 2
        first = (step + 1) % 2
        owner_pos = (pos + n + (2 * way - 1) * hop) % n
        part = (1 - way) * first + way * (1 - first)
        return ring_index(owner_pos, n), part

    def w_copies(unit):
        owner, part = item(unit // 2, unit % 2)
        slot = unit % depth
        start = pl.multiple_of(owner * 2 * chunk + part * chunk, 128)
        return [
            pltpu.make_async_copy(
                w_hbm.at[j, c, :, pl.ds(start, chunk)],
                wbuf.at[slot, j, :, pl.ds(c * chunk, chunk)],
                w_sem.at[slot, j, c],
            )
            for j in range(nodes)
            for c in range(2)
        ]

    def send(step, way, owner, part):
        ref = held.at[owner, part, core]
        return pltpu.make_async_remote_copy(
            src_ref=ref,
            dst_ref=ref,
            send_sem=send_sem.at[step, way],
            recv_sem=recv_sem.at[step, way],
            device_id={"row": right if way == 0 else left},
            device_id_type=pl.DeviceIdType.MESH,
        )

    def pass_over(step, way, owner, part, core_of):
        ref = held.at[owner, part, core_of]
        return pltpu.make_async_remote_copy(
            src_ref=ref,
            dst_ref=ref,
            send_sem=sib_send.at[step, way],
            recv_sem=sib_recv.at[step, way],
            device_id={"freq": other},
            device_id_type=pl.DeviceIdType.MESH,
        )

    own = pltpu.make_async_copy(m_hbm, block, own_sem)
    own.start()
    for unit in range(depth - 1):
        for copy in w_copies(unit):
            copy.start()
    barrier = pltpu.get_barrier_semaphore()
    for hop in range(1, n):
        pl.semaphore_signal(
            barrier, device_id={"row": (me + hop) % n}, device_id_type=pl.DeviceIdType.MESH
        )
    pl.semaphore_signal(barrier, device_id={"freq": other}, device_id_type=pl.DeviceIdType.MESH)
    own.wait()

    def turn(part, f):
        pairs = pl.ds(pl.multiple_of(f * half, half), half)
        for c in range(2):
            piece = block[c, pairs, part * chunk : (part + 1) * chunk]
            held[me, part, f, :, c * half : (c + 1) * half] = piece.T

    turn(0, core)
    turn(1, core)
    pl.semaphore_wait(barrier, n)
    for step in (1, 2):
        for way in (0, 1):
            part = (step + 1) % 2 if way == 0 else 1 - (step + 1) % 2
            send(step, way, me, part).start()
    turn(0, other)
    turn(1, other)
    acc[...] = jnp.zeros_like(acc)

    def compute(unit):
        slot = unit % depth
        owner, part = item(unit // 2, unit % 2)
        for f in range(2):
            rhs[f, :chunk, :] = held[owner, part, f]
            rhs[f, chunk:, :half] = -held[owner, part, f, :, half:]
            rhs[f, chunk:, half:] = held[owner, part, f, :, :half]
        for copy in w_copies(unit):
            copy.wait()

        @pl.when(unit + depth - 1 < units)
        def _():
            for copy in w_copies(unit + depth - 1):
                copy.start()

        tiles = rows // tile

        def one(i, carry):
            j = i // (2 * tiles)
            f = (i // tiles) % 2
            t = i % tiles
            spot = pl.ds(pl.multiple_of(t * tile, tile), tile)
            y = jnp.dot(wbuf[slot, j, spot, :], rhs[f], preferred_element_type=jnp.float32)
            per = chunk // tile
            mine = pl.ds(pl.multiple_of((t % per) * tile, tile), tile)
            m = held[me, t // per, f, mine, :].astype(jnp.float32)
            r, s = m[:, :half], m[:, half:]
            yr, yi = y[:, :half], y[:, half:]
            acc[0, j, f] += jnp.sum((r * yr + s * yi).reshape(tile // 8, 8, half), axis=0)
            acc[1, j, f] += jnp.sum((r * yi - s * yr).reshape(tile // 8, 8, half), axis=0)
            return carry

        lax.fori_loop(0, nodes * 2 * tiles, one, 0, unroll=4)

    def step_body(step, carry):
        @pl.when(step >= 1)
        def _():
            for way in (0, 1):
                owner, part = item(step, way)
                send(step, way, owner, part).wait_recv()

                @pl.when(step + 2 < n)
                def _():
                    send(step + 2, way, owner, part).start()

                pass_over(step, way, owner, part, core).start()
            for way in (0, 1):
                owner, part = item(step, way)
                pass_over(step, way, owner, part, other).wait_recv()

        def each(way, c):
            compute(2 * step + way)
            return c

        lax.fori_loop(0, 2, each, 0)
        return carry

    lax.fori_loop(0, n, step_body, 0)

    lines = 2 * nodes * 2
    forms[:lines, :] = jnp.sum(acc[...], axis=3).reshape(lines, half)
    forms[lines:, :] = jnp.zeros_like(forms[lines:, :])

    def spread(hop):
        return pltpu.make_async_remote_copy(
            src_ref=forms,
            dst_ref=peers.at[hop - 1],
            send_sem=form_send.at[hop - 1],
            recv_sem=form_recv.at[hop - 1],
            device_id={"row": (me + hop) % n},
            device_id_type=pl.DeviceIdType.MESH,
        )

    for hop in range(1, n):
        spread(hop).start()
    def drain(step, carry):
        for way in (0, 1):
            owner, part = item(step, way)
            send(step, way, owner, part).wait_send()
            pass_over(step, way, owner, part, core).wait_send()
        return carry

    lax.fori_loop(1, n, drain, 0)
    total = forms[...]
    for hop in range(1, n):
        spread(hop).wait()
        total += peers[hop - 1]
    twin[0, :lines, :] = total[:lines, :]
    twin[0, lines:, :] = param_ref[...]
    swap = pltpu.make_async_remote_copy(
        src_ref=twin.at[0],
        dst_ref=twin.at[1],
        send_sem=twin_send,
        recv_sem=twin_recv,
        device_id={"freq": other},
        device_id_type=pl.DeviceIdType.MESH,
    )
    swap.start()
    out_ref[0] = twin[0]
    swap.wait()
    out_ref[1] = twin[1]


def ring_forms(screened, elements, node_freq, node_weight):
    nodes, _, rows, ng = screened.shape
    n = lax.axis_size("row")
    npair = elements.shape[1]
    block = elements.shape[2]
    chunk = block // 2
    half = npair // 2
    tile = min(TILE, chunk)
    depth = DEPTH
    lines = 2 * nodes * 2
    spare = -(-2 * nodes // 8) * 8
    params = jnp.concatenate([node_freq, node_weight])
    params = jnp.pad(params, (0, spare - 2 * nodes))
    params = jnp.broadcast_to(params[:, None], (spare, half))
    out = pl.pallas_call(
        functools.partial(ring_kernel, n, nodes, rows, chunk, npair, tile, depth),
        out_shape=jax.ShapeDtypeStruct((2, lines + spare, half), jnp.float32),
        in_specs=[
            pl.BlockSpec(memory_space=pl.ANY),
            pl.BlockSpec(memory_space=pl.ANY),
            pl.BlockSpec(memory_space=pltpu.VMEM),
        ],
        out_specs=pl.BlockSpec(memory_space=pltpu.VMEM),
        scratch_shapes=[
            pltpu.VMEM((2, npair, block), jnp.bfloat16),
            pltpu.VMEM((n, 2, 2, chunk, npair), jnp.bfloat16),
            pltpu.VMEM((depth, nodes, rows, 2 * chunk), jnp.bfloat16),
            pltpu.VMEM((2, 2 * chunk, npair), jnp.bfloat16),
            pltpu.VMEM((2, nodes, 2, 8, half), jnp.float32),
            pltpu.VMEM((lines + spare, half), jnp.float32),
            pltpu.VMEM((n - 1, lines + spare, half), jnp.float32),
            pltpu.VMEM((2, lines + spare, half), jnp.float32),
            pltpu.SemaphoreType.DMA,
            pltpu.SemaphoreType.DMA((depth, nodes, 2)),
            pltpu.SemaphoreType.DMA((n, 2)),
            pltpu.SemaphoreType.DMA((n, 2)),
            pltpu.SemaphoreType.DMA((n, 2)),
            pltpu.SemaphoreType.DMA((n, 2)),
            pltpu.SemaphoreType.DMA((n - 1,)),
            pltpu.SemaphoreType.DMA((n - 1,)),
            pltpu.SemaphoreType.DMA,
            pltpu.SemaphoreType.DMA,
        ],
        compiler_params=pltpu.CompilerParams(
            collective_id=0, has_side_effects=True, vmem_limit_bytes=62 * 1024 * 1024
        ),
    )(screened, elements, params)
    forms = out[:, :lines].reshape(2, 2, nodes, npair).transpose(1, 0, 2, 3)
    forms = forms.reshape(2, 2 * nodes, npair)
    freqs = out[:, lines : lines + nodes, 0].reshape(-1)
    weights = out[:, lines + nodes : lines + 2 * nodes, 0].reshape(-1)
    return forms[0], forms[1], freqs, weights


def per_device(
    screened, elements, node_freq, node_weight, band_energy, energy_grid, pair_state, pair_band
):
    n = lax.axis_size("row")
    two = n >= 4 and n % 2 == 0 and lax.axis_size("freq") == 2
    if two and elements.shape[2] % 256 == 0 and elements.shape[1] % 256 == 0:
        form_re, form_im, freqs, weights = ring_forms(screened, elements, node_freq, node_weight)
        return self_energy(
            form_re, form_im, freqs, weights, band_energy, energy_grid, pair_state, pair_band
        )
    w_real = screened[:, 0]
    w_imag = screened[:, 1]
    npair = elements.shape[1]
    half = npair // lax.axis_size("freq")
    mine = lax.dynamic_slice_in_dim(elements, lax.axis_index("freq") * half, half, 1)
    collected = lax.all_gather(mine, "row", axis=2, tiled=True)
    piece = lax.all_gather(collected, "freq", axis=1, tiled=True)
    part_real = product(w_real, piece[0]) - product(w_imag, piece[1])
    part_imag = product(w_real, piece[1]) + product(w_imag, piece[0])
    stacked = jnp.stack([part_real, part_imag])
    y_real = stacked[0]
    y_imag = stacked[1]
    own_real = elements[0].T.astype(jnp.float32)[None]
    own_imag = elements[1].T.astype(jnp.float32)[None]
    form_re = jnp.sum(own_real * y_real + own_imag * y_imag, axis=1)
    form_im = jnp.sum(own_real * y_imag - own_imag * y_real, axis=1)
    form_re, form_im = lax.psum((form_re, form_im), "row")
    partial_sigma = self_energy(
        form_re, form_im, node_freq, node_weight, band_energy, energy_grid, pair_state, pair_band
    )
    return lax.psum(partial_sigma, "freq")


def solution(mesh):
    in_specs = (
        P(("kpt", "freq"), None, "row", None),
        P(None, "kpt", "row"),
        P("freq"),
        P("freq"),
        P("kpt"),
        P(),
        P("kpt"),
        P("kpt"),
    )
    out_specs = P(None, "kpt", None)
    return jax.shard_map(
        per_device, mesh=mesh, in_specs=in_specs, out_specs=out_specs, check_vma=False
    )
```
